32 devices in a mesh: sub: 16 (over z, x, core), sec: 2 (over y).
Axes of the slice: x: 2, y: 2, z: 4, core: 2. Of those that a mesh axis runs over, the one named last changes fastest.
Arguments:
- image: bfloat16 [16, 2, 512, 512], P('sub', None, 'sec'), may hold values from -6 to 6
- range_offsets: int32 [16, 3, 2, 4], P('sub'), may hold values from 0 to 16
- tap_weights: bfloat16 [16, 3, 2, 128, 8], P('sub'), may hold values from -1.1953125 to 1.1953125
- beam_weights: float32 [16, 3, 2, 4], P('sub'), may hold values from 0.25 to 1
- phase_rates: float32 [16, 3, 2], P('sub'), may hold values from 1 to 40
Outputs:
- merged: bfloat16 [16, 2, 512, 512], P('sub', None, 'sec')
The draws below stay inside these ranges and needn't reach their ends.
All inputs are finite; a program needn't handle non-finite values.
Results may differ from the reference program's by a relative error of at most 0.0043.
Values may be sent and summed in bfloat16 or wider, within the bound.
A program may use at most 64 MiB of HBM per device.

```python
import math
import jax
import jax.numpy as jnp
from jax import lax

RANGE = 512
SECTIONS = 3
BLOCK = 128
TAPS = 8
MARGIN_ROWS = 12
SUBAPERTURES = 16
BEAMS = 512
BLOCKS = 4
N_SUB = 16


def with_ends(drawn, own_key, least, top_value):
    index_at = [jax.random.randint(jax.random.fold_in(own_key, axis), (), 0, length) for axis, length in enumerate(drawn.shape)]
    widest = drawn.shape.index(max(drawn.shape))
    next_to = index_at[:widest] + [(index_at[widest] + 1) % drawn.shape[widest]] + index_at[widest + 1:]
    return drawn.at[tuple(index_at)].set(least).at[tuple(next_to)].set(top_value)


def levels(key, shape, shards, least, largest):
    gain, own = 1.0, jax.random.fold_in(key, 6)
    for position, parts in shards:
        draws = jnp.exp(jax.random.uniform(jax.random.fold_in(own, position), (parts,), jnp.float32, least / len(shards), largest / len(shards)))
        gain = gain * jnp.repeat(draws, shape[position] // parts).reshape([-1 if axis == position else 1 for axis in range(len(shape))])
    return gain


def gaussian(stream_key, extent, deviation, limit, pieces=(), kind=jnp.bfloat16):
    factor_of = levels(stream_key, extent, pieces, -0.22, 0.18) if pieces else 1.0
    values = jax.random.normal(stream_key, extent, jnp.float32) * deviation * factor_of
    return jnp.minimum(jnp.maximum(values, -limit), limit).astype(kind)


def setup_inputs(seed: int = 0) -> dict:
    arg_keys = jax.random.split(jax.random.key(seed), 6)
    image = gaussian(arg_keys[0], (SUBAPERTURES, 2, BEAMS, RANGE), 1.0, 6.0, ((0, 16), (2, 2)))
    range_offsets = with_ends(jax.random.randint(arg_keys[1], (SUBAPERTURES, SECTIONS, 2, BLOCKS), 0, 2 * MARGIN_ROWS - TAPS + 1), jax.random.fold_in(arg_keys[1], 1), 0, 2 * MARGIN_ROWS - TAPS).astype(jnp.int32)
    tap_weights = gaussian(arg_keys[2], (SUBAPERTURES, SECTIONS, 2, BLOCK, TAPS), 0.2, 1.1953125, ((0, 16),))
    beam_weights = jnp.clip(0.25 + 0.75 * jax.random.uniform(arg_keys[3], (SUBAPERTURES, SECTIONS, 2, 4), jnp.float32) ** levels(arg_keys[3], (SUBAPERTURES, SECTIONS, 2, 4), ((0, 16),), -0.2, 0.2), 0.25, 1.0)
    phase_rates = jnp.clip(jnp.exp(math.log(40.0) - 3.6888795 * jax.random.uniform(arg_keys[4], (SUBAPERTURES, SECTIONS, 2), jnp.float32) ** levels(arg_keys[4], (SUBAPERTURES, SECTIONS, 2), ((0, 16),), -0.2, 0.2)), 1.0, 40.0)
    return dict(image=image, range_offsets=range_offsets, tap_weights=tap_weights, beam_weights=beam_weights, phase_rates=phase_rates)


def contribute(child, offsets, tap_weights, beam_weights, phase_rate):
    beams = child.shape[1]
    padded = jnp.pad(child, ((0, 0), (2, 2), (MARGIN_ROWS, MARGIN_ROWS)))
    starts = jnp.arange(RANGE // BLOCK, dtype=jnp.int32) * BLOCK + offsets.astype(jnp.int32)
    windows = jax.vmap(lambda start: lax.dynamic_slice_in_dim(padded, start, BLOCK + TAPS, 2))(starts)
    taps_wide = tap_weights.astype(jnp.float32)
    interp = jnp.zeros(windows.shape[:3] + (BLOCK,), jnp.float32)
    for tap_idx in range(TAPS):
        interp = interp + windows[..., tap_idx:tap_idx + BLOCK].astype(jnp.float32) * taps_wide[:, tap_idx]
    interp = jnp.transpose(interp, (1, 2, 0, 3)).reshape(2, beams + 4, RANGE)
    blended = jnp.zeros((2, beams, RANGE), jnp.float32)
    for angle_idx in range(4):
        blended = blended + beam_weights[angle_idx] * interp[:, 1 + angle_idx:1 + angle_idx + beams]
    beam_idx = jnp.arange(beams, dtype=jnp.int32).astype(jnp.float32)
    range_idx = jnp.arange(RANGE, dtype=jnp.int32).astype(jnp.float32)
    phase = phase_rate * ((beam_idx[:, None] + 1.0) * (range_idx[None, :] + 1.0)) / (RANGE * beams)
    cosine = jnp.cos(phase)
    sine = jnp.sin(phase)
    return jnp.stack([cosine * blended[0] - sine * blended[1], sine * blended[0] + cosine * blended[1]])


def reference(image, range_offsets, tap_weights, beam_weights, phase_rates):
    subimages = image
    positions = jnp.arange(N_SUB, dtype=jnp.int32)
    for section_idx in range(SECTIONS):
        partners = jnp.bitwise_xor(positions, 2 ** section_idx)

        def merge_one(sub_idx, current=subimages, section_idx=section_idx, partners=partners):
            own_part = contribute(current[sub_idx], range_offsets[sub_idx, section_idx, 0],
                                  tap_weights[sub_idx, section_idx, 0], beam_weights[sub_idx, section_idx, 0],
                                  phase_rates[sub_idx, section_idx, 0])
            far_part = contribute(current[partners[sub_idx]], range_offsets[sub_idx, section_idx, 1],
                                  tap_weights[sub_idx, section_idx, 1], beam_weights[sub_idx, section_idx, 1],
                                  phase_rates[sub_idx, section_idx, 1])
            return (own_part + far_part).astype(jnp.bfloat16)

        subimages = lax.map(merge_one, positions)
    return subimages
```

```python
import functools
import math

import jax
import jax.numpy as jnp
from jax import lax
from jax.experimental import pallas as pl
from jax.experimental.pallas import tpu as pltpu
from jax.sharding import PartitionSpec as P

SECTIONS = 3
BLOCK = 128
TAPS = 8
MARGIN_ROWS = 12
TILE = 16
STEP = 2
LAG = 3
MESH = pl.DeviceIdType.MESH


def bounds(tiles):
    inner = list(range(2, tiles - 1, STEP)) + [tiles - 1]
    first = [0] + [v + 1 for v in inner] + [tiles + 1]
    second = [0] + inner + [tiles + 1]
    third = [0] + [v - 1 for v in inner] + [tiles]
    return first, second, third


def sincos_turns(turns):
    x = (turns - jnp.round(turns)) * math.pi
    y = x * x
    s = -1.0 / math.factorial(11)
    for n in (9, 7, 5, 3, 1):
        s = s * y + (1.0 if n % 4 == 1 else -1.0) / math.factorial(n)
    s = s * x
    c = 1.0 / math.factorial(12)
    for n in (10, 8, 6, 4, 2, 0):
        c = c * y + (1.0 if n % 4 == 0 else -1.0) / math.factorial(n)
    return 1.0 - 2.0 * s * s, 2.0 * s * c


def kernel(n_sec, chunks, image_hbm, offsets_hbm, taps_hbm, weights_hbm, rates_hbm, out,
           image, offsets, taps, weights, rates, load_sem, recv0, halo_own, halo_far, s1, r1, s2, r2, band, q, fine, coarse,
           send_sem, recv_sem, hsend_sem, hrecv_sem):
    sub = lax.axis_index("sub")
    sec = lax.axis_index("sec")
    beams, range_len = image.shape[2], image.shape[3]
    tiles = beams // TILE
    blocks = range_len // BLOCK
    partners = []
    for k in range(SECTIONS):
        bit = 1 << k
        partners.append(sub + bit * (1 - 2 * ((sub // bit) % 2)))
    has_low = sec > 0
    has_high = sec < n_sec - 1

    loads = [pltpu.make_async_copy(src, dst, load_sem.at[n]) for n, (src, dst) in enumerate((
        (image_hbm, image), (offsets_hbm, offsets), (taps_hbm, taps), (weights_hbm, weights), (rates_hbm, rates)))]
    for load in loads:
        load.start()

    barrier = pltpu.get_barrier_semaphore()
    for k in range(SECTIONS):
        pl.semaphore_signal(barrier, inc=1, device_id={"sub": partners[k]}, device_id_type=MESH)
    for cond, step in ((has_low, -1), (has_high, 1)):
        @pl.when(cond)
        def _():
            for dst in (sub, partners[0]):
                pl.semaphore_signal(barrier, inc=1, device_id={"sub": dst, "sec": sec + step}, device_id_type=MESH)
    sectors_beside = (sec + n_sec - 1) // n_sec + (2 * (n_sec - 1) - sec) // n_sec
    for k in range(1, SECTIONS):
        for child in range(2):
            for z in range(2):
                for n in range(blocks):
                    q[k, child, z, n, 0:8, :] = jnp.zeros((8, BLOCK), jnp.float32)
                    q[k, child, z, n, beams + 24:beams + 32, :] = jnp.zeros((8, BLOCK), jnp.float32)
    loads[0].wait()
    pl.semaphore_wait(barrier, SECTIONS + 2 * sectors_beside)

    b1, b2, b3 = bounds(tiles)
    outs = (b1, b2, b3)
    ins = ([0] + [v + 1 for v in b1[1:]], b1, b2)

    def halo_copy(side, far):
        rows = pl.ds(beams - TILE, TILE) if side == 0 else pl.ds(0, TILE)
        dst = halo_far if far else halo_own
        return pltpu.make_async_remote_copy(
            src_ref=image.at[0, :, rows, :], dst_ref=dst.at[side],
            send_sem=hsend_sem.at[side, far], recv_sem=hrecv_sem.at[side, far],
            device_id={"sub": partners[0] if far else sub, "sec": sec + (1 if side == 0 else -1)},
            device_id_type=MESH)

    def span(k, j):
        lo, hi = ins[k][j], ins[k][j + 1]
        if k == 0:
            lo, hi = max(lo - 1, 0), min(hi - 1, tiles)
        return lo * TILE, (hi - lo) * TILE

    sources = ((image.at[0], recv0), (s1, r1), (s2, r2))

    def main_copy(k, j):
        lo, size = span(k, j)
        src, dst = sources[k]
        return pltpu.make_async_remote_copy(
            src_ref=src.at[:, pl.ds(lo, size), :], dst_ref=dst.at[:, pl.ds(lo, size), :],
            send_sem=send_sem.at[k, j], recv_sem=recv_sem.at[k, j],
            device_id={"sub": partners[k]}, device_id_type=MESH)

    for side, cond in ((0, has_high), (1, has_low)):
        @pl.when(cond)
        def _():
            for far in (1, 0):
                halo_copy(side, far).start()
    live = [[j for j in range(chunks) if span(k, j)[1]] for k in range(SECTIONS)]
    for j in live[0]:
        main_copy(0, j).start()
    for side, cond in ((0, has_low), (1, has_high)):
        @pl.when(jnp.logical_not(cond))
        def _():
            halo_own[side] = jnp.zeros(halo_own.shape[1:], halo_own.dtype)
            halo_far[side] = jnp.zeros(halo_far.shape[1:], halo_far.dtype)

    sector_start = sec * beams
    total_beams = beams * n_sec

    def prepare(k):
        base = 0 if k == SECTIONS - 1 else -8
        for child in range(2):
            tap = taps[0, k, child].astype(jnp.float32)
            for n in range(blocks):
                lo = max(n * BLOCK - 16, 0)
                hi = min((n + 1) * BLOCK + 16, range_len)
                cols = slice(n * BLOCK, (n + 1) * BLOCK)
                if lo > 0:
                    band[k, child, 0:lo, cols] = jnp.zeros((lo, BLOCK), jnp.bfloat16)
                if hi < range_len:
                    band[k, child, hi:range_len, cols] = jnp.zeros((range_len - hi, BLOCK), jnp.bfloat16)
                which = (lax.broadcasted_iota(jnp.int32, (hi - lo, BLOCK), 0)
                         - lax.broadcasted_iota(jnp.int32, (hi - lo, BLOCK), 1)
                         + (lo - n * BLOCK + MARGIN_ROWS)) - offsets[0, k, child, n]
                value = jnp.zeros((hi - lo, BLOCK), jnp.float32)
                for t in range(TAPS):
                    value = jnp.where(which == t, tap[t:t + 1, :], value)
                band[k, child, lo:hi, cols] = value.astype(jnp.bfloat16)
            per_turn = rates[0, child, k] * (1.0 / (2.0 * math.pi * range_len * total_beams))
            for ref, first, scale in ((fine, sector_start + base + 1, 1), (coarse, 0, TILE)):
                shape = ref.shape[4:]
                beam = (first + scale * lax.broadcasted_iota(jnp.int32, shape, 0)).astype(jnp.float32)
                for n in range(blocks):
                    rng = (lax.broadcasted_iota(jnp.int32, shape, 1) + (n * BLOCK + 1)).astype(jnp.float32)
                    c, s = sincos_turns(beam * rng * per_turn)
                    ref[k, child, 0, n] = c
                    ref[k, child, 1, n] = s

    def interpolate(k, child, data, row):
        rows = data.shape[1]
        flat = data.reshape(2 * rows, range_len)
        for at in range(0, blocks, 2):
            end = min(at + 2, blocks)
            lo, hi = max(at - 1, 0) * BLOCK, min(end + 1, blocks) * BLOCK
            res = jnp.dot(flat[:, lo:hi], band[k, child, lo:hi, at * BLOCK:end * BLOCK],
                          preferred_element_type=jnp.float32)
            for z in range(2):
                for n in range(at, end):
                    q[k, child, z, n, row:row + rows, :] = res[z * rows:(z + 1) * rows, (n - at) * BLOCK:(n - at + 1) * BLOCK]

    def interpolate_chunk(k, child, j):
        ref = sources[k][child]
        lo, size = span(k, j)
        if k == 0:
            halo = halo_own if child == 0 else halo_far
            if j == 0:
                interpolate(k, child, halo[0], 0)
            if size and child == 1:
                interpolate(k, child, ref[:, lo:lo + size, :], lo + TILE)
            if j == chunks - 1:
                interpolate(k, child, halo[1], beams + TILE)
        else:
            interpolate(k, child, ref[:, lo:lo + size, :], lo + 8)

    def combine(k, j):
        base = 0 if k == SECTIONS - 1 else -8
        bw = [[weights[0, k, child, a] for a in range(4)] for child in range(2)]
        first, last = outs[k][j], outs[k][j + 1]

        def tile(t, carry):
            row = pl.multiple_of(t * TILE, TILE)
            view = q.at[k, :, :, :, pl.ds(pl.multiple_of(row + (base + 8), 8), 2 * TILE), :]
            if k < SECTIONS - 1:
                beam = sector_start + base + row + lax.broadcasted_iota(jnp.int32, (TILE, BLOCK), 0)
                inside = (beam >= 0) & (beam < total_beams)
            for n in range(blocks):
                cols = slice(n * BLOCK, (n + 1) * BLOCK)
                total = [None, None]
                for child in range(2):
                    g = []
                    for z in range(2):
                        acc = None
                        for a in range(4):
                            term = bw[child][a] * view[child, z, n, 7 + a:7 + a + TILE, :]
                            acc = term if acc is None else acc + term
                        g.append(acc)
                    cc = coarse[k, child, 0, n, pl.ds(t, 1), :]
                    cs = coarse[k, child, 1, n, pl.ds(t, 1), :]
                    fc = fine[k, child, 0, n]
                    fs = fine[k, child, 1, n]
                    cosine = cc * fc - cs * fs
                    sine = cs * fc + cc * fs
                    re = cosine * g[0] - sine * g[1]
                    im = sine * g[0] + cosine * g[1]
                    total = [re, im] if child == 0 else [total[0] + re, total[1] + im]
                for z in range(2):
                    v = total[z]
                    if k < SECTIONS - 1:
                        v = jnp.where(inside, v, 0.0)
                        (s1, s2)[k][z, pl.ds(row, TILE), cols] = v.astype(jnp.bfloat16)
                    else:
                        out[0, z, pl.ds(row, TILE), cols] = v.astype(jnp.bfloat16)
            return carry

        lax.fori_loop(first, last, tile, 0)

    def step(k, j):
        if k == 0:
            for side, at, cond in ((0, 0, has_low), (1, chunks - 1, has_high)):
                if j == at:
                    @pl.when(cond)
                    def _():
                        for far in (1, 0):
                            halo_copy(side, far).wait_recv()
        if k == 0:
            interpolate_chunk(k, 0, j)
        if j in live[k]:
            main_copy(k, j).wait_recv()
        interpolate_chunk(k, 1, j)
        combine(k, j)
        if k < SECTIONS - 1:
            main_copy(k + 1, j).start()
            if k > 0:
                interpolate_chunk(k + 1, 0, j)

    for load in loads[1:]:
        load.wait()
    prepare(0)
    interpolate(0, 0, image[0], TILE)
    step(0, 0)
    step(0, 1)
    prepare(1)
    for j in range(2, chunks):
        step(0, j)
    interpolate(1, 0, s1[...], 8)
    prepare(2)
    lag = LAG
    for j in range(chunks + lag):
        if j < chunks:
            step(1, j)
        if j >= lag:
            step(2, j - lag)

    for k in range(SECTIONS):
        for j in live[k]:
            main_copy(k, j).wait_send()
    for side, cond in ((0, has_high), (1, has_low)):
        @pl.when(cond)
        def _():
            for far in (1, 0):
                halo_copy(side, far).wait_send()


def solution(mesh):
    n_sec = mesh.shape["sec"]
    def body(image, range_offsets, tap_weights, beam_weights, phase_rates):
        _, _, beams, range_len = image.shape
        chunks = len(bounds(beams // TILE)[0]) - 1
        wide = beams + TILE
        rows = beams + 2 * TILE
        vmem = pl.BlockSpec(memory_space=pltpu.VMEM)
        taps = jnp.swapaxes(tap_weights, 3, 4)
        rates = jnp.swapaxes(phase_rates, 1, 2)
        coarse_rows = -(-(wide // TILE) // 8) * 8
        return pl.pallas_call(
            functools.partial(kernel, n_sec, chunks),
            out_shape=pltpu.VMEM(image.shape, image.dtype),
            in_specs=[pl.BlockSpec(memory_space=pltpu.HBM)] * 5,
            out_specs=vmem,
            scratch_shapes=[
                pltpu.VMEM(image.shape, image.dtype),
                pltpu.SMEM(range_offsets.shape, range_offsets.dtype),
                pltpu.VMEM(taps.shape, taps.dtype),
                pltpu.SMEM(beam_weights.shape, beam_weights.dtype),
                pltpu.SMEM(rates.shape, rates.dtype),
                pltpu.SemaphoreType.DMA((5,)),
                pltpu.VMEM((2, beams, range_len), jnp.bfloat16),
                pltpu.VMEM((2, 2, TILE, range_len), jnp.bfloat16),
                pltpu.VMEM((2, 2, TILE, range_len), jnp.bfloat16),
                pltpu.VMEM((2, wide, range_len), jnp.bfloat16),
                pltpu.VMEM((2, wide, range_len), jnp.bfloat16),
                pltpu.VMEM((2, wide, range_len), jnp.bfloat16),
                pltpu.VMEM((2, wide, range_len), jnp.bfloat16),
                pltpu.VMEM((SECTIONS, 2, range_len, range_len), jnp.bfloat16),
                pltpu.VMEM((SECTIONS, 2, 2, range_len // BLOCK, rows, BLOCK), jnp.float32),
                pltpu.VMEM((SECTIONS, 2, 2, range_len // BLOCK, TILE, BLOCK), jnp.float32),
                pltpu.VMEM((SECTIONS, 2, 2, range_len // BLOCK, coarse_rows, BLOCK), jnp.float32),
                pltpu.SemaphoreType.DMA((SECTIONS, chunks)),
                pltpu.SemaphoreType.DMA((SECTIONS, chunks)),
                pltpu.SemaphoreType.DMA((2, 2)),
                pltpu.SemaphoreType.DMA((2, 2)),
            ],
            compiler_params=pltpu.CompilerParams(
                collective_id=0, has_side_effects=True),
        )(image, range_offsets, taps, beam_weights, rates)

    in_specs = (
        P("sub", None, "sec", None),
        P("sub", None, None, None),
        P("sub", None, None, None, None),
        P("sub", None, None, None),
        P("sub", None, None),
    )
    return jax.shard_map(body, mesh=mesh, in_specs=in_specs,
                         out_specs=P("sub", None, "sec", None), check_vma=False)
```
